8 devices in a mesh: dp: 2 (over z, y), tp: 4 (over x, core).
Axes of the slice: x: 2, y: 2, z: 1, core: 2. Of those that a mesh axis runs over, the one named last changes fastest.
Arguments:
- tokens_in: bfloat16 [2, 256, 1664], P('dp'), parts along dimension 0
- ln_scale: bfloat16 [2, 1664], replicated
- w_query: bfloat16 [2, 1664, 1664], P(None, None, 'tp')
- w_key: bfloat16 [2, 1664, 1664], P(None, None, 'tp')
- w_value: bfloat16 [2, 1664, 1664], P(None, None, 'tp')
- q_scale: bfloat16 [2, 104], replicated
- k_scale: bfloat16 [2, 104], replicated
- w_out: bfloat16 [2, 1664, 1664], P(None, 'tp')
- b_out: bfloat16 [2, 1664], replicated
- w_up: bfloat16 [2, 1664, 8192], P(None, None, 'tp')
- b_up: bfloat16 [2, 8192], P(None, 'tp')
- w_down: bfloat16 [2, 8192, 1664], P(None, 'tp')
- b_down: bfloat16 [2, 1664], replicated
Outputs:
- output: bfloat16 [2, 256, 1664], P('dp'), parts along dimension 0
There are 2 independent parts. The reference program is written for one: setup_inputs(seed, part) draws one part's arguments, and reference() takes and returns one part's arrays. A program takes and returns all parts, laid end to end along the dimension named above; an argument that names none is the same for every part.
All inputs are finite; a program needn't handle non-finite values.
Results may differ from the reference program's by a relative error of at most 0.012433.
Values are sent between devices in bfloat16 or wider.
A program may use at most 1 GiB of HBM per device.

```python
import jax
import jax.numpy as jnp
from jax import lax

IMAGES = 1
SEQ_LEN = 256
MODEL_DIM = 1664
NUM_HEADS = 16
HEAD_DIM = 104
MLP_DIM = 8192
LAYERS = 2
LN_EPS = 1e-6


def setup_inputs(seed: int = 0, part: int = 0) -> dict:
    base_key = jax.random.key(seed)
    part_key = jax.random.fold_in(base_key, part)
    key_list = jax.random.split(base_key, 12)
    hidden = NUM_HEADS * HEAD_DIM

    def normal(rng_key, arr_shape, spread, offset):
        std_draw = jax.random.normal(rng_key, arr_shape, jnp.float32)
        return (offset + spread * std_draw).astype(jnp.bfloat16)

    return {
        "tokens_in": normal(part_key, (IMAGES, SEQ_LEN, MODEL_DIM), 1.0, 0.0),
        "ln_scale": normal(key_list[0], (LAYERS, MODEL_DIM), 0.3, 1.0),
        "w_query": normal(key_list[1], (LAYERS, MODEL_DIM, hidden), MODEL_DIM ** -0.5, 0.0),
        "w_key": normal(key_list[2], (LAYERS, MODEL_DIM, hidden), MODEL_DIM ** -0.5, 0.0),
        "w_value": normal(key_list[3], (LAYERS, MODEL_DIM, hidden), MODEL_DIM ** -0.5, 0.0),
        "q_scale": normal(key_list[4], (LAYERS, HEAD_DIM), 0.3, 1.5),
        "k_scale": normal(key_list[5], (LAYERS, HEAD_DIM), 0.3, 1.5),
        "w_out": normal(key_list[6], (LAYERS, hidden, MODEL_DIM), hidden ** -0.5, 0.0),
        "b_out": normal(key_list[7], (LAYERS, MODEL_DIM), 0.5, 0.0),
        "w_up": normal(key_list[8], (LAYERS, MODEL_DIM, MLP_DIM), MODEL_DIM ** -0.5, 0.0),
        "b_up": normal(key_list[9], (LAYERS, MLP_DIM), 0.5, 0.0),
        "w_down": normal(key_list[10], (LAYERS, MLP_DIM, MODEL_DIM), MLP_DIM ** -0.5, 0.0),
        "b_down": normal(key_list[11], (LAYERS, MODEL_DIM), 0.5, 0.0),
    }


def layer_norm(values, scale_vec):
    mean_val = jnp.mean(values, axis=-1, keepdims=True)
    centered = values - mean_val
    variance = jnp.mean(centered * centered, axis=-1, keepdims=True)
    return centered * lax.rsqrt(variance + LN_EPS) * scale_vec.astype(jnp.float32)


def one_layer(tokens_in, ln_scale, w_query, w_key, w_value, q_scale, k_scale, w_out, b_out, w_up, b_up, w_down, b_down):
    n_tokens = IMAGES * SEQ_LEN
    residual = tokens_in.reshape(n_tokens, MODEL_DIM).astype(jnp.float32)
    normed = layer_norm(residual, ln_scale).astype(jnp.bfloat16)

    def project(weight):
        projected = jnp.dot(normed, weight, preferred_element_type=jnp.float32)
        return projected.reshape(IMAGES, SEQ_LEN, NUM_HEADS, HEAD_DIM)

    queries = layer_norm(project(w_query), q_scale).astype(jnp.bfloat16)
    keys_all = layer_norm(project(w_key), k_scale).astype(jnp.bfloat16)
    values_all = project(w_value).astype(jnp.bfloat16)

    def attend(operands):
        q_img, k_img, v_img = operands
        scores = jnp.einsum("qhd,khd->hqk", q_img.astype(jnp.float32), k_img.astype(jnp.float32)) * HEAD_DIM ** -0.5
        attn_prob = jax.nn.softmax(scores, axis=-1).astype(jnp.bfloat16)
        mixed_val = jnp.einsum("hqk,khd->qhd", attn_prob.astype(jnp.float32), v_img.astype(jnp.float32))
        return mixed_val.astype(jnp.bfloat16)

    attended = lax.map(attend, (queries, keys_all, values_all)).reshape(n_tokens, NUM_HEADS * HEAD_DIM)
    attn_part = jnp.dot(attended, w_out, preferred_element_type=jnp.float32)
    pre_act = jnp.dot(normed, w_up, preferred_element_type=jnp.float32) + b_up.astype(jnp.float32)
    activated = jax.nn.gelu(pre_act, approximate=True).astype(jnp.bfloat16)
    mlp_part = jnp.dot(activated, w_down, preferred_element_type=jnp.float32)
    summed = residual + b_out.astype(jnp.float32) + b_down.astype(jnp.float32) + attn_part + mlp_part
    return summed.astype(jnp.bfloat16).reshape(IMAGES, SEQ_LEN, MODEL_DIM)


def reference(tokens_in, ln_scale, w_query, w_key, w_value, q_scale, k_scale, w_out, b_out, w_up, b_up, w_down, b_down):
    def step_fn(state_in, params):
        return one_layer(state_in, *params), None

    encoded, _ = lax.scan(step_fn, tokens_in, (ln_scale, w_query, w_key, w_value, q_scale, k_scale, w_out, b_out, w_up, b_up, w_down, b_down))
    return encoded
```

```python
import functools

import jax
import jax.numpy as jnp
from jax import lax
from jax.experimental import pallas as pl
from jax.experimental.pallas import tpu as pltpu
from jax.sharding import PartitionSpec as P

LN_EPS = 1e-6
MESH = pl.DeviceIdType.MESH
F32 = jnp.float32
BF16 = jnp.bfloat16

T = 256
D = 1664
HD = 104
NH = 4
HW = NH * HD
FF = 2048
CH = 128
OWN = CH // 2
WIN = 256
WIN0 = (0, 0, 128, 256)
OFF = (0, 104, 80, 56)
COLS = ((0, 512), (512, 512), (1024, 640))
UPB = ((0, 512), (512, 512), (1024, 512), (1536, 512))
NB = len(COLS)


def kernel(x_hbm, lns_ref, wq_hbm, wk_hbm, wv_hbm, qs_ref, ks_ref, wo_hbm, bo_ref, wu_hbm, bu_ref, wd_hbm, bd_ref,
           out_hbm,
           x_s, wq_s, wk_s, wv_s, wo_s, wu_s, wd_s,
           h_s, proj_s, q4_s, k4_s, v4_s, o_s, act_s, acc_s,
           dsend, drecv, xsend, xrecv, y_s,
           wsem, iosem, dss, drs, xss, xrs, fss, frs):
    tp = lax.axis_index("tp")
    core = lax.rem(tp, 2)
    sib = tp + 1 - 2 * core
    cross = lax.rem(tp + 2, 4)

    xcopy = pltpu.make_async_copy(x_hbm.at[0], x_s, iosem.at[0])
    xcopy.start()
    wcopies = {}
    nsem = [0]

    def wcopy(name, l, src, dst):
        wcopies[(name, l)] = pltpu.make_async_copy(src, dst, wsem.at[nsem[0]])
        nsem[0] += 1

    for l in range(2):
        wcopy("k", l, wk_hbm.at[l], wk_s.at[l])
        wcopy("v", l, wv_hbm.at[l], wv_s.at[l])
        wcopy("q", l, wq_hbm.at[l], wq_s.at[l])
        for i, (n0, nn) in enumerate(UPB):
            wcopy(("u", i), l, wu_hbm.at[l, :, pl.ds(n0, nn)], wu_s.at[l, :, pl.ds(n0, nn)])
        for i, (n0, nn) in enumerate(COLS):
            wcopy(("o", i), l, wo_hbm.at[l, :, pl.ds(n0, nn)], wo_s.at[l, :, pl.ds(n0, nn)])
            wcopy(("d", i), l, wd_hbm.at[l, :, pl.ds(n0, nn)], wd_s.at[l, :, pl.ds(n0, nn)])
    for (name, l), cp in wcopies.items():
        if l == 0:
            cp.start()
    waited = set()

    def need(name, l):
        if (name, l) not in waited:
            waited.add((name, l))
            wcopies[(name, l)].wait()

    barrier = pltpu.get_barrier_semaphore()
    for peer in (sib, cross):
        pl.semaphore_signal(barrier, inc=1, device_id={"tp": peer}, device_id_type=MESH)

    lane = lax.broadcasted_iota(jnp.int32, (8, WIN), 1)
    masks = [(lane >= OFF[i]) & (lane < OFF[i] + HD) for i in range(NH)]

    def mask_of(i, rows):
        lane_r = lax.broadcasted_iota(jnp.int32, (rows, WIN), 1)
        return (lane_r >= OFF[i]) & (lane_r < OFF[i] + HD)

    def gain_windows(ref, l):
        g = ref[l : l + 1, :].astype(F32)
        g = jnp.concatenate([g, jnp.zeros((1, WIN - HD), F32)], axis=1)
        g8 = jnp.broadcast_to(g, (8, WIN))
        return [(pltpu.roll(g8, OFF[i], 1) if OFF[i] else g8)[0:1, :] for i in range(NH)]

    def ln_rows(src, l, rows):
        v = src[rows, :].astype(F32)
        mean = jnp.sum(v, axis=1, keepdims=True) * (1.0 / D)
        cen = v - mean
        var = jnp.sum(cen * cen, axis=1, keepdims=True) * (1.0 / D)
        g = lns_ref[l : l + 1, :].astype(F32)
        h_s[rows, :] = (cen * lax.rsqrt(var + LN_EPS) * g).astype(BF16)

    def head_norm(dst, gains, rows, n):
        for i in range(NH):
            w = proj_s[rows, pl.ds(WIN0[i], WIN)]
            m = mask_of(i, n)
            w = jnp.where(m, w, 0.0)
            mean = jnp.sum(w, axis=1, keepdims=True) * (1.0 / HD)
            cen = jnp.where(m, w - mean, 0.0)
            var = jnp.sum(cen * cen, axis=1, keepdims=True) * (1.0 / HD)
            dst[i, rows, :] = (cen * lax.rsqrt(var + LN_EPS) * gains[i]).astype(BF16)

    def project(w_s, l, rows):
        proj_s[rows, pl.ds(0, HW)] = jnp.dot(h_s[rows, :], w_s[l], preferred_element_type=F32)

    def do_k(l, rows, n, gk):
        need("k", l)
        project(wk_s, l, rows)
        head_norm(k4_s, gk, rows, n)

    def do_v(l, rows, n):
        need("v", l)
        project(wv_s, l, rows)
        for i in range(NH):
            w = proj_s[rows, pl.ds(WIN0[i], WIN)]
            v4_s[i, rows, :] = jnp.where(mask_of(i, n), w, 0.0).astype(BF16)

    def do_q(l, rows, n, gq):
        need("q", l)
        project(wq_s, l, rows)
        head_norm(q4_s, gq, rows, n)

    def attend(rows):
        os = []
        for i in range(NH):
            s = lax.dot_general(q4_s[i, rows, :], k4_s[i], (((1,), (1,)), ((), ())), preferred_element_type=F32)
            s = s * (HD ** -0.5)
            e = jnp.exp(s - jnp.max(s, axis=1, keepdims=True))
            p = (e * (1.0 / jnp.sum(e, axis=1, keepdims=True))).astype(BF16)
            os.append(jnp.dot(p, v4_s[i], preferred_element_type=F32))
        lo = [o[:, 0:128] for o in os]
        hi = [o[:, 128:256] for o in os]
        o_s[rows, 0:128] = (lo[0] + lo[1]).astype(BF16)
        o_s[rows, 128:256] = (hi[1] + lo[2]).astype(BF16)
        o_s[rows, 256:384] = (hi[2] + lo[3]).astype(BF16)
        o_s[rows, 384:512] = hi[3].astype(BF16)

    def do_up(l, rows):
        for i, (n0, nn) in enumerate(UPB):
            need(("u", i), l)
            z = jnp.dot(h_s[rows, :], wu_s[l, :, pl.ds(n0, nn)], preferred_element_type=F32)
            z = z + bu_ref[l : l + 1, pl.ds(n0, nn)].astype(F32)
            t = jnp.tanh(z * (0.7978845608028654 + (0.7978845608028654 * 0.044715) * (z * z)))
            act_s[rows, pl.ds(n0, nn)] = (0.5 * z * (1.0 + t)).astype(BF16)

    def mlp_block(l, c, rows, b):
        n0, nn = COLS[b]
        need(("d", b), l)
        return jnp.dot(act_s[rows, :], wd_s[l, :, pl.ds(n0, nn)], preferred_element_type=F32)

    def attn_block(l, c, rows, b):
        n0, nn = COLS[b]
        need(("o", b), l)
        return jnp.dot(o_s[rows, pl.ds(0, HW)], wo_s[l, :, pl.ds(n0, nn)], preferred_element_type=F32)

    own_off = pl.multiple_of(core * OWN, OWN)
    sib_off = pl.multiple_of((1 - core) * OWN, OWN)

    def d_rdma(l, c, b):
        n0, nn = COLS[b]
        return pltpu.make_async_remote_copy(
            src_ref=dsend.at[l, c, :, pl.ds(n0, nn)], dst_ref=drecv.at[l, c, :, pl.ds(n0, nn)],
            send_sem=dss.at[l, c, b], recv_sem=drs.at[l, c, b], device_id={"tp": sib}, device_id_type=MESH)

    def x_rdma(l, c, b):
        n0, nn = COLS[b]
        return pltpu.make_async_remote_copy(
            src_ref=xsend.at[l, c, :, pl.ds(n0, nn)], dst_ref=xrecv.at[l, c, :, pl.ds(n0, nn)],
            send_sem=xss.at[l, c, b], recv_sem=xrs.at[l, c, b], device_id={"tp": cross}, device_id_type=MESH)

    def f_rdma(l, c, b):
        n0, nn = COLS[b]
        view = y_s.at[l, pl.ds(pl.multiple_of(c * CH + core * OWN, OWN), OWN), pl.ds(n0, nn)]
        return pltpu.make_async_remote_copy(
            src_ref=view, dst_ref=view,
            send_sem=fss.at[l, c, b], recv_sem=frs.at[l, c, b], device_id={"tp": sib}, device_id_type=MESH)

    def emit_block(l, c, b, part):
        n0, nn = COLS[b]
        acc_s[c, :, pl.ds(n0, nn)] = part
        dsend[l, c, :, pl.ds(n0, nn)] = acc_s[c, pl.ds(sib_off, OWN), pl.ds(n0, nn)].astype(BF16)
        d_rdma(l, c, b).start()

    def cross_block(l, c, b):
        n0, nn = COLS[b]
        d_rdma(l, c, b).wait_recv()
        s = acc_s[c, pl.ds(own_off, OWN), pl.ds(n0, nn)] + drecv[l, c, :, pl.ds(n0, nn)].astype(F32)
        xsend[l, c, :, pl.ds(n0, nn)] = s.astype(BF16)
        x_rdma(l, c, b).start()

    def finish_block(l, c, b):
        n0, nn = COLS[b]
        x_rdma(l, c, b).wait_recv()
        r = pl.ds(pl.multiple_of(c * CH + core * OWN, OWN), OWN)
        res = x_s[r, pl.ds(n0, nn)] if l == 0 else y_s[0, r, pl.ds(n0, nn)]
        base = res.astype(F32) + bo_ref[l : l + 1, pl.ds(n0, nn)].astype(F32) + bd_ref[l : l + 1, pl.ds(n0, nn)].astype(F32)
        both = xsend[l, c, :, pl.ds(n0, nn)].astype(F32) + xrecv[l, c, :, pl.ds(n0, nn)].astype(F32)
        y_s[l, r, pl.ds(n0, nn)] = (base + both).astype(BF16)
        f_rdma(l, c, b).start()

    rows = [pl.ds(0, CH), pl.ds(CH, CH)]
    proj_s[:, pl.ds(HW, 512 - HW)] = jnp.zeros((T, 512 - HW), F32)

    gk = gain_windows(ks_ref, 0)
    gq = gain_windows(qs_ref, 0)
    xcopy.wait()
    ln_rows(x_s, 0, rows[0])
    ln_rows(x_s, 0, rows[1])
    do_k(0, pl.ds(0, T), T, gk)
    do_v(0, pl.ds(0, T), T)
    do_q(0, rows[0], CH, gq)
    attend(rows[0])
    do_up(0, rows[0])
    pl.semaphore_wait(barrier, 2)
    for b in range(NB):
        emit_block(0, 0, b, mlp_block(0, 0, rows[0], b) + attn_block(0, 0, rows[0], b))
        if b >= 1:
            cross_block(0, 0, b - 1)
    for (name, l), cp in wcopies.items():
        if l == 1:
            cp.start()
    do_q(0, rows[1], CH, gq)
    cross_block(0, 0, NB - 1)
    attend(rows[1])
    do_up(0, rows[1])
    for b in range(NB):
        emit_block(0, 1, b, mlp_block(0, 1, rows[1], b) + attn_block(0, 1, rows[1], b))
        if b >= 1:
            cross_block(0, 1, b - 1)
    gk = gain_windows(ks_ref, 1)
    gq = gain_windows(qs_ref, 1)
    cross_block(0, 1, NB - 1)

    for b in range(NB):
        finish_block(0, 0, b)
    for b in range(NB):
        f_rdma(0, 0, b).wait_recv()
    y0 = y_s.at[0]
    ln_rows(y0, 1, rows[0])
    do_k(1, rows[0], CH, gk)
    do_v(1, rows[0], CH)
    do_q(1, rows[0], CH, gq)
    do_up(1, rows[0])
    for b in range(NB):
        acc_s[0, :, pl.ds(*COLS[b])] = mlp_block(1, 0, rows[0], b)
    for b in range(NB):
        finish_block(0, 1, b)
    for b in range(NB):
        f_rdma(0, 1, b).wait_recv()
    ln_rows(y0, 1, rows[1])
    do_k(1, rows[1], CH, gk)
    do_v(1, rows[1], CH)
    attend(rows[0])
    for b in range(NB):
        emit_block(1, 0, b, acc_s[0, :, pl.ds(*COLS[b])] + attn_block(1, 0, rows[0], b))
        if b >= 1:
            cross_block(1, 0, b - 1)
    do_q(1, rows[1], CH, gq)
    cross_block(1, 0, NB - 1)
    attend(rows[1])
    do_up(1, rows[1])
    for b in range(NB):
        emit_block(1, 1, b, mlp_block(1, 1, rows[1], b) + attn_block(1, 1, rows[1], b))
        if b >= 1:
            cross_block(1, 1, b - 1)
    cross_block(1, 1, NB - 1)

    def out_own(c):
        r = pl.ds(pl.multiple_of(c * CH + core * OWN, OWN), OWN)
        return pltpu.make_async_copy(y_s.at[1, r], out_hbm.at[0, r], iosem.at[1 + 2 * c])

    def out_sib(c):
        r = pl.ds(pl.multiple_of(c * CH + (1 - core) * OWN, OWN), OWN)
        return pltpu.make_async_copy(y_s.at[1, r], out_hbm.at[0, r], iosem.at[2 + 2 * c])

    for c in range(2):
        for b in range(NB):
            finish_block(1, c, b)
        out_own(c).start()
        for b in range(NB):
            f_rdma(1, c, b).wait_recv()
        out_sib(c).start()
    for l in range(2):
        for c in range(2):
            for b in range(NB):
                d_rdma(l, c, b).wait_send()
                x_rdma(l, c, b).wait_send()
                f_rdma(l, c, b).wait_send()
    for c in range(2):
        out_own(c).wait()
        out_sib(c).wait()


def solution(mesh):
    col_spec = P(None, None, "tp")
    row_spec = P(None, "tp", None)
    in_specs = (P("dp", None, None), P(), col_spec, col_spec, col_spec, P(), P(), row_spec, P(), col_spec, P(None, "tp"), row_spec, P())
    any_spec = pl.BlockSpec(memory_space=pl.ANY)
    vmem_spec = pl.BlockSpec(memory_space=pltpu.VMEM)
    nw = 2 * (3 + len(UPB) + 2 * NB)
    call = pl.pallas_call(
        kernel,
        out_shape=jax.ShapeDtypeStruct((1, T, D), BF16),
        in_specs=[any_spec, vmem_spec, any_spec, any_spec, any_spec, vmem_spec, vmem_spec, any_spec, vmem_spec, any_spec, vmem_spec, any_spec, vmem_spec],
        out_specs=any_spec,
        scratch_shapes=[
            pltpu.VMEM((T, D), BF16),
            pltpu.VMEM((2, D, HW), BF16),
            pltpu.VMEM((2, D, HW), BF16),
            pltpu.VMEM((2, D, HW), BF16),
            pltpu.VMEM((2, HW, D), BF16),
            pltpu.VMEM((2, D, FF), BF16),
            pltpu.VMEM((2, FF, D), BF16),
            pltpu.VMEM((T, D), BF16),
            pltpu.VMEM((T, 512), F32),
            pltpu.VMEM((NH, T, WIN), BF16),
            pltpu.VMEM((NH, T, WIN), BF16),
            pltpu.VMEM((NH, T, WIN), BF16),
            pltpu.VMEM((T, 512), BF16),
            pltpu.VMEM((T, FF), BF16),
            pltpu.VMEM((2, CH, D), F32),
            pltpu.VMEM((2, 2, OWN, D), BF16),
            pltpu.VMEM((2, 2, OWN, D), BF16),
            pltpu.VMEM((2, 2, OWN, D), BF16),
            pltpu.VMEM((2, 2, OWN, D), BF16),
            pltpu.VMEM((2, T, D), BF16),
            pltpu.SemaphoreType.DMA((nw,)),
            pltpu.SemaphoreType.DMA((5,)),
            pltpu.SemaphoreType.DMA((2, 2, NB)),
            pltpu.SemaphoreType.DMA((2, 2, NB)),
            pltpu.SemaphoreType.DMA((2, 2, NB)),
            pltpu.SemaphoreType.DMA((2, 2, NB)),
            pltpu.SemaphoreType.DMA((2, 2, NB)),
            pltpu.SemaphoreType.DMA((2, 2, NB)),
        ],
        compiler_params=pltpu.CompilerParams(collective_id=0, has_side_effects=True, vmem_limit_bytes=62 * 1024 * 1024),
        name="vit_pair",
    )

    def per_device(*args):
        return call(*args)

    return jax.shard_map(per_device, mesh=mesh, in_specs=in_specs, out_specs=P("dp", None, None), check_vma=False)
```

```python
import functools

import jax
import jax.numpy as jnp
from jax import lax
from jax.experimental import pallas as pl
from jax.experimental.pallas import tpu as pltpu
from jax.sharding import PartitionSpec as P

LN_EPS = 1e-6
MESH = pl.DeviceIdType.MESH
F32 = jnp.float32
BF16 = jnp.bfloat16

T = 256
D = 1664
HD = 104
NH = 4
HW = NH * HD
FF = 2048
CH = 128
OWN = CH // 2
COLS = ((0, 512), (512, 512), (1024, 640))
UPB = ((0, 512), (512, 512), (1024, 512), (1536, 512))
NB = len(COLS)


def kernel(x_hbm, lns_ref, wq_hbm, wk_hbm, wv_hbm, qs_ref, ks_ref, wo_hbm, bo_ref, wu_hbm, bu_ref, wd_hbm, bd_ref,
           out_hbm,
           x_s, wt_s, wo_s, wu_s, wd_s,
           h_s, ot_s, q4_s, k4_s, v4_s, o_s, act_s, acc_s,
           dsend, drecv, xsend, xrecv, y_s,
           wsem, iosem, dss, drs, xss, xrs, fss, frs):
    tp = lax.axis_index("tp")
    core = lax.rem(tp, 2)
    sib = tp + 1 - 2 * core
    cross = lax.rem(tp + 2, 4)

    xcopy = pltpu.make_async_copy(x_hbm.at[0], x_s, iosem.at[0])
    xcopy.start()
    wcopies = {}
    nsem = [0]

    def wcopy(name, l, src, dst):
        wcopies[(name, l)] = pltpu.make_async_copy(src, dst, wsem.at[nsem[0]])
        nsem[0] += 1

    for l in range(2):
        wcopy("k", l, wk_hbm.at[l], wt_s.at[l, pl.ds(0, HW)])
        wcopy("v", l, wv_hbm.at[l], wt_s.at[l, pl.ds(HW, HW)])
        wcopy("q", l, wq_hbm.at[l], wt_s.at[l, pl.ds(2 * HW, HW)])
        for i, (n0, nn) in enumerate(UPB):
            wcopy(("u", i), l, wu_hbm.at[l, :, pl.ds(n0, nn)], wu_s.at[l, :, pl.ds(n0, nn)])
        for i, (n0, nn) in enumerate(COLS):
            wcopy(("o", i), l, wo_hbm.at[l, :, pl.ds(n0, nn)], wo_s.at[l, :, pl.ds(n0, nn)])
            wcopy(("d", i), l, wd_hbm.at[l, :, pl.ds(n0, nn)], wd_s.at[l, :, pl.ds(n0, nn)])
    for (name, l), cp in wcopies.items():
        if l == 0:
            cp.start()
    waited = set()

    def need(name, l):
        if (name, l) not in waited:
            waited.add((name, l))
            wcopies[(name, l)].wait()

    barrier = pltpu.get_barrier_semaphore()
    for peer in (sib, cross):
        pl.semaphore_signal(barrier, inc=1, device_id={"tp": peer}, device_id_type=MESH)

    def gain_cols(ref, l):
        g = ref[l : l + 1, :].astype(F32)
        g = jnp.concatenate([g, jnp.zeros((1, 128 - HD), F32)], axis=1)
        g = jnp.broadcast_to(g, (128, 128)).T[0:HD, :]
        return jnp.concatenate([g, g], axis=1)

    def ln_rows(src, l, rows):
        v = src[rows, :].astype(F32)
        mean = jnp.sum(v, axis=1, keepdims=True) * (1.0 / D)
        cen = v - mean
        var = jnp.sum(cen * cen, axis=1, keepdims=True) * (1.0 / D)
        g = lns_ref[l : l + 1, :].astype(F32)
        h_s[rows, :] = (cen * lax.rsqrt(var + LN_EPS) * g).astype(BF16)

    def project(l, r0, rows):
        return lax.dot_general(wt_s[l, pl.ds(r0, HW), :], h_s[rows, :], (((1,), (1,)), ((), ())), preferred_element_type=F32)

    def head_norm(dst, pt, gains, rows, n):
        for i in range(NH):
            w = pt[i * HD : (i + 1) * HD, :]
            mean = jnp.sum(w, axis=0, keepdims=True) * (1.0 / HD)
            cen = w - mean
            var = jnp.sum(cen * cen, axis=0, keepdims=True) * (1.0 / HD)
            dst[i, :, rows] = (cen * lax.rsqrt(var + LN_EPS) * gains[:, 0:n]).astype(BF16)

    def do_k(l, rows, n, gk):
        need("k", l)
        head_norm(k4_s, project(l, 0, rows), gk, rows, n)

    def do_v(l, rows, n):
        need("v", l)
        pt = project(l, HW, rows)
        for i in range(NH):
            v4_s[i, :, rows] = pt[i * HD : (i + 1) * HD, :].astype(BF16)

    def do_q(l, rows, n, gq):
        need("q", l)
        head_norm(q4_s, project(l, 2 * HW, rows), gq, rows, n)

    def attend(rows):
        for i in range(NH):
            s = lax.dot_general(k4_s[i], q4_s[i, :, rows], (((0,), (0,)), ((), ())), preferred_element_type=F32)
            s = s * (HD ** -0.5)
            e = jnp.exp(s - jnp.max(s, axis=0, keepdims=True))
            p = (e * (1.0 / jnp.sum(e, axis=0, keepdims=True))).astype(BF16)
            ot_s[pl.ds(i * HD, HD), :] = jnp.dot(v4_s[i], p, preferred_element_type=F32)
        o_s[rows, :] = ot_s[...].T.astype(BF16)

    def do_up(l, rows):
        for i, (n0, nn) in enumerate(UPB):
            need(("u", i), l)
            z = jnp.dot(h_s[rows, :], wu_s[l, :, pl.ds(n0, nn)], preferred_element_type=F32)
            z = z + bu_ref[l : l + 1, pl.ds(n0, nn)].astype(F32)
            t = jnp.tanh(z * (0.7978845608028654 + (0.7978845608028654 * 0.044715) * (z * z)))
            act_s[rows, pl.ds(n0, nn)] = (0.5 * z * (1.0 + t)).astype(BF16)

    def mlp_block(l, c, rows, b):
        n0, nn = COLS[b]
        need(("d", b), l)
        return jnp.dot(act_s[rows, :], wd_s[l, :, pl.ds(n0, nn)], preferred_element_type=F32)

    def attn_block(l, c, rows, b):
        n0, nn = COLS[b]
        need(("o", b), l)
        return jnp.dot(o_s[rows, pl.ds(0, HW)], wo_s[l, :, pl.ds(n0, nn)], preferred_element_type=F32)

    own_off = pl.multiple_of(core * OWN, OWN)
    sib_off = pl.multiple_of((1 - core) * OWN, OWN)

    def d_rdma(l, c, b):
        n0, nn = COLS[b]
        return pltpu.make_async_remote_copy(
            src_ref=dsend.at[l, c, :, pl.ds(n0, nn)], dst_ref=drecv.at[l, c, :, pl.ds(n0, nn)],
            send_sem=dss.at[l, c, b], recv_sem=drs.at[l, c, b], device_id={"tp": sib}, device_id_type=MESH)

    def x_rdma(l, c, b):
        n0, nn = COLS[b]
        return pltpu.make_async_remote_copy(
            src_ref=xsend.at[l, c, :, pl.ds(n0, nn)], dst_ref=xrecv.at[l, c, :, pl.ds(n0, nn)],
            send_sem=xss.at[l, c, b], recv_sem=xrs.at[l, c, b], device_id={"tp": cross}, device_id_type=MESH)

    def f_rdma(l, c, b):
        n0, nn = COLS[b]
        view = y_s.at[l, pl.ds(pl.multiple_of(c * CH + core * OWN, OWN), OWN), pl.ds(n0, nn)]
        return pltpu.make_async_remote_copy(
            src_ref=view, dst_ref=view,
            send_sem=fss.at[l, c, b], recv_sem=frs.at[l, c, b], device_id={"tp": sib}, device_id_type=MESH)

    def emit_block(l, c, b, part):
        n0, nn = COLS[b]
        acc_s[c, :, pl.ds(n0, nn)] = part
        dsend[l, c, :, pl.ds(n0, nn)] = acc_s[c, pl.ds(sib_off, OWN), pl.ds(n0, nn)].astype(BF16)
        d_rdma(l, c, b).start()

    def cross_block(l, c, b):
        n0, nn = COLS[b]
        d_rdma(l, c, b).wait_recv()
        s = acc_s[c, pl.ds(own_off, OWN), pl.ds(n0, nn)] + drecv[l, c, :, pl.ds(n0, nn)].astype(F32)
        xsend[l, c, :, pl.ds(n0, nn)] = s.astype(BF16)
        x_rdma(l, c, b).start()

    def finish_block(l, c, b):
        n0, nn = COLS[b]
        x_rdma(l, c, b).wait_recv()
        r = pl.ds(pl.multiple_of(c * CH + core * OWN, OWN), OWN)
        res = x_s[r, pl.ds(n0, nn)] if l == 0 else y_s[0, r, pl.ds(n0, nn)]
        base = res.astype(F32) + bo_ref[l : l + 1, pl.ds(n0, nn)].astype(F32) + bd_ref[l : l + 1, pl.ds(n0, nn)].astype(F32)
        both = xsend[l, c, :, pl.ds(n0, nn)].astype(F32) + xrecv[l, c, :, pl.ds(n0, nn)].astype(F32)
        y_s[l, r, pl.ds(n0, nn)] = (base + both).astype(BF16)
        f_rdma(l, c, b).start()

    rows = [pl.ds(0, CH), pl.ds(CH, CH)]
    ot_s[pl.ds(HW, 512 - HW), :] = jnp.zeros((512 - HW, CH), F32)

    gk = gain_cols(ks_ref, 0)
    gq = gain_cols(qs_ref, 0)
    xcopy.wait()
    ln_rows(x_s, 0, rows[0])
    ln_rows(x_s, 0, rows[1])
    do_k(0, pl.ds(0, T), T, gk)
    do_v(0, pl.ds(0, T), T)
    do_q(0, pl.ds(0, T), T, gq)
    attend(rows[0])
    do_up(0, rows[0])
    pl.semaphore_wait(barrier, 2)
    for b in range(NB):
        emit_block(0, 0, b, mlp_block(0, 0, rows[0], b) + attn_block(0, 0, rows[0], b))
        if b >= 1:
            cross_block(0, 0, b - 1)
    for (name, l), cp in wcopies.items():
        if l == 1:
            cp.start()
    cross_block(0, 0, NB - 1)
    attend(rows[1])
    do_up(0, rows[1])
    for b in range(NB):
        emit_block(0, 1, b, mlp_block(0, 1, rows[1], b) + attn_block(0, 1, rows[1], b))
        if b >= 1:
            cross_block(0, 1, b - 1)
    gk = gain_cols(ks_ref, 1)
    gq = gain_cols(qs_ref, 1)
    cross_block(0, 1, NB - 1)

    for b in range(NB):
        finish_block(0, 0, b)
    for b in range(NB):
        f_rdma(0, 0, b).wait_recv()
    y0 = y_s.at[0]
    ln_rows(y0, 1, rows[0])
    do_k(1, rows[0], CH, gk)
    do_v(1, rows[0], CH)
    do_q(1, rows[0], CH, gq)
    do_up(1, rows[0])
    for b in range(NB):
        acc_s[0, :, pl.ds(*COLS[b])] = mlp_block(1, 0, rows[0], b)
    for b in range(NB):
        finish_block(0, 1, b)
    for b in range(NB):
        f_rdma(0, 1, b).wait_recv()
    ln_rows(y0, 1, rows[1])
    do_k(1, rows[1], CH, gk)
    do_v(1, rows[1], CH)
    attend(rows[0])
    for b in range(NB):
        emit_block(1, 0, b, acc_s[0, :, pl.ds(*COLS[b])] + attn_block(1, 0, rows[0], b))
        if b >= 1:
            cross_block(1, 0, b - 1)
    do_q(1, rows[1], CH, gq)
    cross_block(1, 0, NB - 1)
    attend(rows[1])
    do_up(1, rows[1])
    for b in range(NB):
        emit_block(1, 1, b, mlp_block(1, 1, rows[1], b) + attn_block(1, 1, rows[1], b))
        if b >= 1:
            cross_block(1, 1, b - 1)
    cross_block(1, 1, NB - 1)

    def out_own(c):
        r = pl.ds(pl.multiple_of(c * CH + core * OWN, OWN), OWN)
        return pltpu.make_async_copy(y_s.at[1, r], out_hbm.at[0, r], iosem.at[1 + 2 * c])

    def out_sib(c):
        r = pl.ds(pl.multiple_of(c * CH + (1 - core) * OWN, OWN), OWN)
        return pltpu.make_async_copy(y_s.at[1, r], out_hbm.at[0, r], iosem.at[2 + 2 * c])

    for c in range(2):
        for b in range(NB):
            finish_block(1, c, b)
        out_own(c).start()
        for b in range(NB):
            f_rdma(1, c, b).wait_recv()
        out_sib(c).start()
    for l in range(2):
        for c in range(2):
            for b in range(NB):
                d_rdma(l, c, b).wait_send()
                x_rdma(l, c, b).wait_send()
                f_rdma(l, c, b).wait_send()
    for c in range(2):
        out_own(c).wait()
        out_sib(c).wait()


def solution(mesh):
    col_spec = P(None, None, "tp")
    row_spec = P(None, "tp", None)
    in_specs = (P("dp", None, None), P(), col_spec, col_spec, col_spec, P(), P(), row_spec, P(), col_spec, P(None, "tp"), row_spec, P())
    any_spec = pl.BlockSpec(memory_space=pl.ANY)
    vmem_spec = pl.BlockSpec(memory_space=pltpu.VMEM)
    nw = 2 * (3 + len(UPB) + 2 * NB)
    call = pl.pallas_call(
        kernel,
        out_shape=jax.ShapeDtypeStruct((1, T, D), BF16),
        in_specs=[any_spec, vmem_spec, any_spec, any_spec, any_spec, vmem_spec, vmem_spec, any_spec, vmem_spec, any_spec, vmem_spec, any_spec, vmem_spec],
        out_specs=any_spec,
        scratch_shapes=[
            pltpu.VMEM((T, D), BF16),
            pltpu.VMEM((2, 3 * HW, D), BF16),
            pltpu.VMEM((2, HW, D), BF16),
            pltpu.VMEM((2, D, FF), BF16),
            pltpu.VMEM((2, FF, D), BF16),
            pltpu.VMEM((T, D), BF16),
            pltpu.VMEM((512, CH), F32),
            pltpu.VMEM((NH, HD, T), BF16),
            pltpu.VMEM((NH, HD, T), BF16),
            pltpu.VMEM((NH, HD, T), BF16),
            pltpu.VMEM((T, 512), BF16),
            pltpu.VMEM((T, FF), BF16),
            pltpu.VMEM((2, CH, D), F32),
            pltpu.VMEM((2, 2, OWN, D), BF16),
            pltpu.VMEM((2, 2, OWN, D), BF16),
            pltpu.VMEM((2, 2, OWN, D), BF16),
            pltpu.VMEM((2, 2, OWN, D), BF16),
            pltpu.VMEM((2, T, D), BF16),
            pltpu.SemaphoreType.DMA((nw,)),
            pltpu.SemaphoreType.DMA((5,)),
            pltpu.SemaphoreType.DMA((2, 2, NB)),
            pltpu.SemaphoreType.DMA((2, 2, NB)),
            pltpu.SemaphoreType.DMA((2, 2, NB)),
            pltpu.SemaphoreType.DMA((2, 2, NB)),
            pltpu.SemaphoreType.DMA((2, 2, NB)),
            pltpu.SemaphoreType.DMA((2, 2, NB)),
        ],
        compiler_params=pltpu.CompilerParams(collective_id=0, has_side_effects=True, vmem_limit_bytes=62 * 1024 * 1024),
        name="vit_pair",
    )

    def per_device(x, lns, wq, wk, wv, *rest):
        return call(x, lns, *(jnp.swapaxes(w, 1, 2) for w in (wq, wk, wv)), *rest)

    return jax.shard_map(per_device, mesh=mesh, in_specs=in_specs, out_specs=P("dp", None, None), check_vma=False)
```

```python
import functools

import jax
import jax.numpy as jnp
from jax import lax
from jax.experimental import pallas as pl
from jax.experimental.pallas import tpu as pltpu
from jax.sharding import PartitionSpec as P

LN_EPS = 1e-6
MESH = pl.DeviceIdType.MESH
F32 = jnp.float32
BF16 = jnp.bfloat16

T = 256
D = 1664
HD = 104
NH = 4
HW = NH * HD
FF = 2048
CH = 128
OWN = CH // 2
COLS = ((0, 512), (512, 512), (1024, 640))
UPB = ((0, 512), (512, 512), (1024, 512), (1536, 512))
NB = len(COLS)


def kernel(x_hbm, lns_hbm, wq_hbm, wk_hbm, wv_hbm, qs_hbm, ks_hbm, wo_hbm, bo_hbm, wu_hbm, bu_hbm, wd_hbm, bd_hbm,
           out_ref,
           lns_ref, qs_ref, ks_ref, bo_ref, bu_ref, bd_ref, x_s, wt_s, wo_s, wu_s, wd_s,
           h_s, ot_s, q4_s, k4_s, v4_s, o_s, act_s, acc_s,
           dsend, drecv, xsend, xrecv, y_s,
           wsem, iosem, dss, drs, xss, xrs, fss, frs):
    tp = lax.axis_index("tp")
    core = lax.rem(tp, 2)
    sib = tp + 1 - 2 * core
    cross = lax.rem(tp + 2, 4)

    xcopy = pltpu.make_async_copy(x_hbm.at[0], x_s, iosem.at[0])
    xcopy.start()
    smalls = [
        pltpu.make_async_copy(src, dst, iosem.at[1 + i])
        for i, (src, dst) in enumerate(
            ((lns_hbm, lns_ref), (ks_hbm, ks_ref), (qs_hbm, qs_ref), (bu_hbm, bu_ref), (bo_hbm, bo_ref), (bd_hbm, bd_ref)))
    ]
    for cp in smalls:
        cp.start()
    barrier = pltpu.get_barrier_semaphore()
    for peer in (sib, cross):
        pl.semaphore_signal(barrier, inc=1, device_id={"tp": peer}, device_id_type=MESH)
    wcopies = {}
    nsem = [0]

    def wcopy(name, l, src, dst):
        wcopies[(name, l)] = pltpu.make_async_copy(src, dst, wsem.at[nsem[0]])
        nsem[0] += 1

    for l in range(2):
        wcopy("k", l, wk_hbm.at[l], wt_s.at[l, pl.ds(0, HW)])
        wcopy("v", l, wv_hbm.at[l], wt_s.at[l, pl.ds(HW, HW)])
        wcopy("q", l, wq_hbm.at[l], wt_s.at[l, pl.ds(2 * HW, HW)])
        for i, (n0, nn) in enumerate(UPB):
            wcopy(("u", i), l, wu_hbm.at[l, :, pl.ds(n0, nn)], wu_s.at[l, :, pl.ds(n0, nn)])
        for i, (n0, nn) in enumerate(COLS):
            wcopy(("o", i), l, wo_hbm.at[l, :, pl.ds(n0, nn)], wo_s.at[l, :, pl.ds(n0, nn)])
            wcopy(("d", i), l, wd_hbm.at[l, :, pl.ds(n0, nn)], wd_s.at[l, :, pl.ds(n0, nn)])
    for (name, l), cp in wcopies.items():
        if l == 0:
            cp.start()
    waited = set()

    def need(name, l):
        if (name, l) not in waited:
            waited.add((name, l))
            wcopies[(name, l)].wait()

    def gain_cols(ref, l):
        g = ref[l : l + 1, :].astype(F32)
        g = jnp.concatenate([g, jnp.zeros((1, 128 - HD), F32)], axis=1)
        g = jnp.broadcast_to(g, (128, 128)).T[0:HD, :]
        return jnp.concatenate([g, g], axis=1)

    def ln_rows(src, l, rows):
        v = src[rows, :].astype(F32)
        mean = jnp.sum(v, axis=1, keepdims=True) * (1.0 / D)
        cen = v - mean
        var = jnp.sum(cen * cen, axis=1, keepdims=True) * (1.0 / D)
        g = lns_ref[l : l + 1, :].astype(F32)
        h_s[rows, :] = (cen * lax.rsqrt(var + LN_EPS) * g).astype(BF16)

    def project(l, r0, nr, rows):
        return lax.dot_general(wt_s[l, pl.ds(r0, nr), :], h_s[rows, :], (((1,), (1,)), ((), ())), preferred_element_type=F32)

    def head_norm(dst, i, w, gains, rows, n):
        mean = jnp.sum(w, axis=0, keepdims=True) * (1.0 / HD)
        cen = w - mean
        var = jnp.sum(cen * cen, axis=0, keepdims=True) * (1.0 / HD)
        dst[i, :, rows] = (cen * lax.rsqrt(var + LN_EPS) * gains[:, 0:n]).astype(BF16)

    def place(kind, i, w, l, rows, n):
        if kind == 0:
            head_norm(k4_s, i, w, gain_cols(ks_ref, l), rows, n)
        elif kind == 1:
            v4_s[i, :, rows] = w.astype(BF16)
        else:
            head_norm(q4_s, i, w, gain_cols(qs_ref, l), rows, n)

    def heads(l, r0, nr, rows, n):
        half = nr // 2
        parts = [project(l, r0, half, rows), project(l, r0 + half, half, rows)]
        for g in range(r0 // HD, (r0 + nr) // HD):
            p, off = divmod(g * HD - r0, half)
            place(g // NH, g % NH, parts[p][off : off + HD, :], l, rows, n)

    def do_kvq(l, rows, n):
        for name in "kvq":
            need(name, l)
        heads(l, 0, 3 * HW, rows, n)

    def do_kv(l, rows, n):
        for name in "kv":
            need(name, l)
        heads(l, 0, 2 * HW, rows, n)

    def do_q(l, rows, n):
        need("q", l)
        heads(l, 2 * HW, HW, rows, n)

    def attend(rows):
        for i in range(NH):
            s = lax.dot_general(k4_s[i], q4_s[i, :, rows], (((0,), (0,)), ((), ())), preferred_element_type=F32)
            s = s * (HD ** -0.5)
            e = jnp.exp(s - jnp.max(s, axis=0, keepdims=True))
            p = (e * (1.0 / jnp.sum(e, axis=0, keepdims=True))).astype(BF16)
            ot_s[pl.ds(i * HD, HD), :] = jnp.dot(v4_s[i], p, preferred_element_type=F32)
        o_s[rows, :] = ot_s[...].T.astype(BF16)

    def do_up(l, rows):
        for i, (n0, nn) in enumerate(UPB):
            need(("u", i), l)
            z = jnp.dot(h_s[rows, :], wu_s[l, :, pl.ds(n0, nn)], preferred_element_type=F32)
            z = z + bu_ref[l : l + 1, pl.ds(n0, nn)].astype(F32)
            t = jnp.tanh(z * (0.7978845608028654 + (0.7978845608028654 * 0.044715) * (z * z)))
            act_s[rows, pl.ds(n0, nn)] = (0.5 * z * (1.0 + t)).astype(BF16)

    def mlp_block(l, c, rows, b):
        n0, nn = COLS[b]
        need(("d", b), l)
        return jnp.dot(act_s[rows, :], wd_s[l, :, pl.ds(n0, nn)], preferred_element_type=F32)

    def attn_block(l, c, rows, b):
        n0, nn = COLS[b]
        need(("o", b), l)
        return jnp.dot(o_s[rows, pl.ds(0, HW)], wo_s[l, :, pl.ds(n0, nn)], preferred_element_type=F32)

    own_off = pl.multiple_of(core * OWN, OWN)
    sib_off = pl.multiple_of((1 - core) * OWN, OWN)

    def d_rdma(l, c, b):
        n0, nn = COLS[b]
        return pltpu.make_async_remote_copy(
            src_ref=dsend.at[l, c, :, pl.ds(n0, nn)], dst_ref=drecv.at[l, c, :, pl.ds(n0, nn)],
            send_sem=dss.at[l, c, b], recv_sem=drs.at[l, c, b], device_id={"tp": sib}, device_id_type=MESH)

    def x_rdma(l, c, b):
        n0, nn = COLS[b]
        return pltpu.make_async_remote_copy(
            src_ref=xsend.at[l, c, :, pl.ds(n0, nn)], dst_ref=xrecv.at[l, c, :, pl.ds(n0, nn)],
            send_sem=xss.at[l, c, b], recv_sem=xrs.at[l, c, b], device_id={"tp": cross}, device_id_type=MESH)

    def f_rdma(l, c, b):
        n0, nn = COLS[b]
        view = y_s.at[l, pl.ds(pl.multiple_of(c * CH + core * OWN, OWN), OWN), pl.ds(n0, nn)]
        return pltpu.make_async_remote_copy(
            src_ref=view, dst_ref=view,
            send_sem=fss.at[l, c, b], recv_sem=frs.at[l, c, b], device_id={"tp": sib}, device_id_type=MESH)

    def emit_block(l, c, b, part):
        n0, nn = COLS[b]
        acc_s[c, :, pl.ds(n0, nn)] = part
        dsend[l, c, :, pl.ds(n0, nn)] = acc_s[c, pl.ds(sib_off, OWN), pl.ds(n0, nn)].astype(BF16)
        d_rdma(l, c, b).start()

    def cross_block(l, c, b):
        n0, nn = COLS[b]
        d_rdma(l, c, b).wait_recv()
        s = acc_s[c, pl.ds(own_off, OWN), pl.ds(n0, nn)] + drecv[l, c, :, pl.ds(n0, nn)].astype(F32)
        xsend[l, c, :, pl.ds(n0, nn)] = s.astype(BF16)
        x_rdma(l, c, b).start()

    def finish_block(l, c, b):
        n0, nn = COLS[b]
        x_rdma(l, c, b).wait_recv()
        r = pl.ds(pl.multiple_of(c * CH + core * OWN, OWN), OWN)
        res = x_s[r, pl.ds(n0, nn)] if l == 0 else y_s[0, r, pl.ds(n0, nn)]
        base = res.astype(F32) + bo_ref[l : l + 1, pl.ds(n0, nn)].astype(F32) + bd_ref[l : l + 1, pl.ds(n0, nn)].astype(F32)
        both = xsend[l, c, :, pl.ds(n0, nn)].astype(F32) + xrecv[l, c, :, pl.ds(n0, nn)].astype(F32)
        y = (base + both).astype(BF16)
        y_s[l, r, pl.ds(n0, nn)] = y
        if l == 1:
            out_ref[0, r, pl.ds(n0, nn)] = y
        f_rdma(l, c, b).start()

    rows = [pl.ds(0, CH), pl.ds(CH, CH)]
    ot_s[pl.ds(HW, 512 - HW), :] = jnp.zeros((512 - HW, CH), F32)

    xcopy.wait()
    for cp in smalls:
        cp.wait()
    ln_rows(x_s, 0, rows[0])
    ln_rows(x_s, 0, rows[1])
    do_kvq(0, pl.ds(0, T), T)
    attend(rows[0])
    do_up(0, rows[0])
    pl.semaphore_wait(barrier, 2)
    for b in range(NB):
        emit_block(0, 0, b, mlp_block(0, 0, rows[0], b) + attn_block(0, 0, rows[0], b))
        if b >= 1:
            cross_block(0, 0, b - 1)
    for (name, l), cp in wcopies.items():
        if l == 1:
            cp.start()
    cross_block(0, 0, NB - 1)
    attend(rows[1])
    do_up(0, rows[1])
    for b in range(NB):
        emit_block(0, 1, b, mlp_block(0, 1, rows[1], b) + attn_block(0, 1, rows[1], b))
        if b >= 1:
            cross_block(0, 1, b - 1)
    cross_block(0, 1, NB - 1)

    for b in range(NB):
        finish_block(0, 0, b)
    for b in range(NB):
        f_rdma(0, 0, b).wait_recv()
    y0 = y_s.at[0]
    ln_rows(y0, 1, rows[0])
    do_kvq(1, rows[0], CH)
    do_up(1, rows[0])
    for b in range(NB):
        acc_s[0, :, pl.ds(*COLS[b])] = mlp_block(1, 0, rows[0], b)
    for b in range(NB):
        finish_block(0, 1, b)
    for b in range(NB):
        f_rdma(0, 1, b).wait_recv()
    ln_rows(y0, 1, rows[1])
    do_kv(1, rows[1], CH)
    attend(rows[0])
    for b in range(NB):
        emit_block(1, 0, b, acc_s[0, :, pl.ds(*COLS[b])] + attn_block(1, 0, rows[0], b))
        if b >= 1:
            cross_block(1, 0, b - 1)
    do_q(1, rows[1], CH)
    cross_block(1, 0, NB - 1)
    attend(rows[1])
    do_up(1, rows[1])
    for b in range(NB):
        emit_block(1, 1, b, mlp_block(1, 1, rows[1], b) + attn_block(1, 1, rows[1], b))
        if b >= 1:
            cross_block(1, 1, b - 1)
    cross_block(1, 1, NB - 1)

    for c in range(2):
        for b in range(NB):
            finish_block(1, c, b)
        for b in range(NB):
            n0, nn = COLS[b]
            f_rdma(1, c, b).wait_recv()
            r = pl.ds(pl.multiple_of(c * CH + (1 - core) * OWN, OWN), OWN)
            out_ref[0, r, pl.ds(n0, nn)] = y_s[1, r, pl.ds(n0, nn)]
    for l in range(2):
        for c in range(2):
            for b in range(NB):
                d_rdma(l, c, b).wait_send()
                x_rdma(l, c, b).wait_send()
                f_rdma(l, c, b).wait_send()


def solution(mesh):
    col_spec = P(None, None, "tp")
    row_spec = P(None, "tp", None)
    in_specs = (P("dp", None, None), P(), col_spec, col_spec, col_spec, P(), P(), row_spec, P(), col_spec, P(None, "tp"), row_spec, P())
    any_spec = pl.BlockSpec(memory_space=pl.ANY)
    vmem_spec = pl.BlockSpec(memory_space=pltpu.VMEM)
    nw = 2 * (3 + len(UPB) + 2 * NB)
    call = pl.pallas_call(
        kernel,
        out_shape=pltpu.VMEM((1, T, D), BF16),
        in_specs=[any_spec] * 13,
        out_specs=vmem_spec,
        scratch_shapes=[
            pltpu.VMEM((2, D), BF16),
            pltpu.VMEM((2, HD), BF16),
            pltpu.VMEM((2, HD), BF16),
            pltpu.VMEM((2, D), BF16),
            pltpu.VMEM((2, FF), BF16),
            pltpu.VMEM((2, D), BF16),
            pltpu.VMEM((T, D), BF16),
            pltpu.VMEM((2, 3 * HW, D), BF16),
            pltpu.VMEM((2, HW, D), BF16),
            pltpu.VMEM((2, D, FF), BF16),
            pltpu.VMEM((2, FF, D), BF16),
            pltpu.VMEM((T, D), BF16),
            pltpu.VMEM((512, CH), F32),
            pltpu.VMEM((NH, HD, T), BF16),
            pltpu.VMEM((NH, HD, T), BF16),
            pltpu.VMEM((NH, HD, T), BF16),
            pltpu.VMEM((T, 512), BF16),
            pltpu.VMEM((T, FF), BF16),
            pltpu.VMEM((2, CH, D), F32),
            pltpu.VMEM((2, 2, OWN, D), BF16),
            pltpu.VMEM((2, 2, OWN, D), BF16),
            pltpu.VMEM((2, 2, OWN, D), BF16),
            pltpu.VMEM((2, 2, OWN, D), BF16),
            pltpu.VMEM((2, T, D), BF16),
            pltpu.SemaphoreType.DMA((nw,)),
            pltpu.SemaphoreType.DMA((7,)),
            pltpu.SemaphoreType.DMA((2, 2, NB)),
            pltpu.SemaphoreType.DMA((2, 2, NB)),
            pltpu.SemaphoreType.DMA((2, 2, NB)),
            pltpu.SemaphoreType.DMA((2, 2, NB)),
            pltpu.SemaphoreType.DMA((2, 2, NB)),
            pltpu.SemaphoreType.DMA((2, 2, NB)),
        ],
        compiler_params=pltpu.CompilerParams(collective_id=0, has_side_effects=True, vmem_limit_bytes=54 * 1024 * 1024),
        name="vit_pair",
    )

    def per_device(x, lns, wq, wk, wv, *rest):
        return call(x, lns, *(jnp.swapaxes(w, 1, 2) for w in (wq, wk, wv)), *rest)

    return jax.shard_map(per_device, mesh=mesh, in_specs=in_specs, out_specs=P("dp", None, None), check_vma=False)
```

```python
import functools

import jax
import jax.numpy as jnp
from jax import lax
from jax.experimental import pallas as pl
from jax.experimental.pallas import tpu as pltpu
from jax.sharding import PartitionSpec as P

LN_EPS = 1e-6
MESH = pl.DeviceIdType.MESH
F32 = jnp.float32
BF16 = jnp.bfloat16

T = 256
D = 1664
HD = 104
NH = 4
HW = NH * HD
FF = 2048
CH = 128
OWN = CH // 2
COLS = ((0, 512), (512, 512), (1024, 640))
UPB = ((0, 512), (512, 512), (1024, 512), (1536, 512))
NB = len(COLS)


def kernel(x_hbm, lns_hbm, wq_hbm, wk_hbm, wv_hbm, qs_hbm, ks_hbm, wo_hbm, bo_hbm, wu_hbm, bu_hbm, wd_hbm, bd_hbm,
           out_ref,
           lns_ref, qs_ref, ks_ref, bo_ref, bu_ref, bd_ref, x_s, wt_s, wo_s, wu_s, wd_s,
           h_s, ot_s, s_s, p_s, q4_s, k4_s, v4_s, o_s, act_s, acc_s,
           dsend, drecv, xsend, xrecv, y_s,
           wsem, iosem, dss, drs, xss, xrs, fss, frs):
    tp = lax.axis_index("tp")
    core = lax.rem(tp, 2)
    sib = tp + 1 - 2 * core
    cross = lax.rem(tp + 2, 4)

    xcopy = pltpu.make_async_copy(x_hbm.at[0], x_s, iosem.at[0])
    xcopy.start()
    smalls = [
        pltpu.make_async_copy(src, dst, iosem.at[1 + i])
        for i, (src, dst) in enumerate(
            ((lns_hbm, lns_ref), (ks_hbm, ks_ref), (qs_hbm, qs_ref), (bu_hbm, bu_ref), (bo_hbm, bo_ref), (bd_hbm, bd_ref)))
    ]
    for cp in smalls:
        cp.start()
    barrier = pltpu.get_barrier_semaphore()
    for peer in (sib, cross):
        pl.semaphore_signal(barrier, inc=1, device_id={"tp": peer}, device_id_type=MESH)
    wcopies = {}
    nsem = [0]

    def wcopy(name, l, src, dst):
        wcopies[(name, l)] = pltpu.make_async_copy(src, dst, wsem.at[nsem[0]])
        nsem[0] += 1

    for l in range(2):
        wcopy("k", l, wk_hbm.at[l], wt_s.at[l, pl.ds(0, HW)])
        wcopy("q", l, wq_hbm.at[l], wt_s.at[l, pl.ds(2 * HW, HW)])
        wcopy("v", l, wv_hbm.at[l], wt_s.at[l, pl.ds(HW, HW)])
        for i, (n0, nn) in enumerate(UPB):
            wcopy(("u", i), l, wu_hbm.at[l, :, pl.ds(n0, nn)], wu_s.at[l, :, pl.ds(n0, nn)])
        for i, (n0, nn) in enumerate(COLS):
            wcopy(("o", i), l, wo_hbm.at[l, :, pl.ds(n0, nn)], wo_s.at[l, :, pl.ds(n0, nn)])
            wcopy(("d", i), l, wd_hbm.at[l, :, pl.ds(n0, nn)], wd_s.at[l, :, pl.ds(n0, nn)])
    for (name, l), cp in wcopies.items():
        if l == 0:
            cp.start()
    waited = set()

    def need(name, l):
        if (name, l) not in waited:
            waited.add((name, l))
            wcopies[(name, l)].wait()

    def gain_cols(ref, l):
        g = ref[l : l + 1, :].astype(F32)
        g = jnp.concatenate([g, jnp.zeros((1, 128 - HD), F32)], axis=1)
        g = jnp.broadcast_to(g, (128, 128)).T[0:HD, :]
        return jnp.concatenate([g, g], axis=1)

    def ln_rows(src, l, rows):
        v = src[rows, :].astype(F32)
        mean = jnp.sum(v, axis=1, keepdims=True) * (1.0 / D)
        cen = v - mean
        var = jnp.sum(cen * cen, axis=1, keepdims=True) * (1.0 / D)
        g = lns_ref[l : l + 1, :].astype(F32)
        h_s[rows, :] = (cen * lax.rsqrt(var + LN_EPS) * g).astype(BF16)

    def project(l, r0, nr, rows):
        return lax.dot_general(wt_s[l, pl.ds(r0, nr), :], h_s[rows, :], (((1,), (1,)), ((), ())), preferred_element_type=F32)

    def head_norm(w, gains, n):
        mean = jnp.sum(w, axis=0, keepdims=True) * (1.0 / HD)
        cen = w - mean
        var = jnp.sum(cen * cen, axis=0, keepdims=True) * (1.0 / HD)
        normed = cen * lax.rsqrt(var + LN_EPS) * gains[:, 0:n]
        return jnp.concatenate([normed, jnp.zeros((128 - HD, n), F32)], axis=0)

    def heads(l, kind, rows, n):
        need("kvq"[kind], l)
        half = HW // 2
        parts = [project(l, kind * HW, half, rows), project(l, kind * HW + half, half, rows)]
        if kind != 1:
            gains = gain_cols(ks_ref if kind == 0 else qs_ref, l)
        for i in range(NH):
            p, off = divmod(i * HD, half)
            w = parts[p][off : off + HD, :]
            if kind == 0:
                k4_s[i, rows, :] = head_norm(w, gains, n).T.astype(BF16)
            elif kind == 1:
                v4_s[i, :, rows] = w.astype(BF16)
            else:
                q4_s[i, :, rows] = head_norm(w, gains, n).astype(BF16)

    def scores(rows, keys):
        for i in range(NH):
            s_s[i, keys, :] = jnp.dot(k4_s[i, keys, :], q4_s[i, :, rows], preferred_element_type=F32)

    def mix(rows):
        for i in range(NH):
            s = s_s[i] * (HD ** -0.5)
            e = jnp.exp(s - jnp.max(s, axis=0, keepdims=True))
            p_s[i] = (e * (1.0 / jnp.sum(e, axis=0, keepdims=True))).astype(BF16)
        for i in range(NH):
            ot_s[pl.ds(i * HD, HD), :] = jnp.dot(v4_s[i], p_s[i], preferred_element_type=F32)
        o_s[rows, :] = ot_s[...].T.astype(BF16)

    def do_up(l, rows):
        for i, (n0, nn) in enumerate(UPB):
            need(("u", i), l)
            z = jnp.dot(h_s[rows, :], wu_s[l, :, pl.ds(n0, nn)], preferred_element_type=F32)
            z = z + bu_ref[l : l + 1, pl.ds(n0, nn)].astype(F32)
            t = jnp.tanh(z * (0.7978845608028654 + (0.7978845608028654 * 0.044715) * (z * z)))
            act_s[rows, pl.ds(n0, nn)] = (0.5 * z * (1.0 + t)).astype(BF16)

    def mlp_block(l, c, rows, b):
        n0, nn = COLS[b]
        need(("d", b), l)
        return jnp.dot(act_s[rows, :], wd_s[l, :, pl.ds(n0, nn)], preferred_element_type=F32)

    def attn_block(l, c, rows, b):
        n0, nn = COLS[b]
        need(("o", b), l)
        return jnp.dot(o_s[rows, pl.ds(0, HW)], wo_s[l, :, pl.ds(n0, nn)], preferred_element_type=F32)

    own_off = pl.multiple_of(core * OWN, OWN)
    sib_off = pl.multiple_of((1 - core) * OWN, OWN)

    def d_rdma(l, c, b):
        n0, nn = COLS[b]
        return pltpu.make_async_remote_copy(
            src_ref=dsend.at[l, c, :, pl.ds(n0, nn)], dst_ref=drecv.at[l, c, :, pl.ds(n0, nn)],
            send_sem=dss.at[l, c, b], recv_sem=drs.at[l, c, b], device_id={"tp": sib}, device_id_type=MESH)

    def x_rdma(l, c, b):
        n0, nn = COLS[b]
        return pltpu.make_async_remote_copy(
            src_ref=xsend.at[l, c, :, pl.ds(n0, nn)], dst_ref=xrecv.at[l, c, :, pl.ds(n0, nn)],
            send_sem=xss.at[l, c, b], recv_sem=xrs.at[l, c, b], device_id={"tp": cross}, device_id_type=MESH)

    def f_rdma(l, c, b):
        n0, nn = COLS[b]
        view = y_s.at[l, pl.ds(pl.multiple_of(c * CH + core * OWN, OWN), OWN), pl.ds(n0, nn)]
        return pltpu.make_async_remote_copy(
            src_ref=view, dst_ref=view,
            send_sem=fss.at[l, c, b], recv_sem=frs.at[l, c, b], device_id={"tp": sib}, device_id_type=MESH)

    def emit_block(l, c, b, part):
        n0, nn = COLS[b]
        acc_s[c, :, pl.ds(n0, nn)] = part
        dsend[l, c, :, pl.ds(n0, nn)] = acc_s[c, pl.ds(sib_off, OWN), pl.ds(n0, nn)].astype(BF16)
        d_rdma(l, c, b).start()

    def cross_block(l, c, b):
        n0, nn = COLS[b]
        d_rdma(l, c, b).wait_recv()
        s = acc_s[c, pl.ds(own_off, OWN), pl.ds(n0, nn)] + drecv[l, c, :, pl.ds(n0, nn)].astype(F32)
        xsend[l, c, :, pl.ds(n0, nn)] = s.astype(BF16)
        x_rdma(l, c, b).start()

    def finish_block(l, c, b):
        n0, nn = COLS[b]
        x_rdma(l, c, b).wait_recv()
        r = pl.ds(pl.multiple_of(c * CH + core * OWN, OWN), OWN)
        res = x_s[r, pl.ds(n0, nn)] if l == 0 else y_s[0, r, pl.ds(n0, nn)]
        base = res.astype(F32) + bo_ref[l : l + 1, pl.ds(n0, nn)].astype(F32) + bd_ref[l : l + 1, pl.ds(n0, nn)].astype(F32)
        both = xsend[l, c, :, pl.ds(n0, nn)].astype(F32) + xrecv[l, c, :, pl.ds(n0, nn)].astype(F32)
        y = (base + both).astype(BF16)
        y_s[l, r, pl.ds(n0, nn)] = y
        if l == 1:
            out_ref[0, r, pl.ds(n0, nn)] = y
        f_rdma(l, c, b).start()

    rows = [pl.ds(0, CH), pl.ds(CH, CH)]
    ot_s[pl.ds(HW, 512 - HW), :] = jnp.zeros((512 - HW, CH), F32)

    xcopy.wait()
    for cp in smalls:
        cp.wait()
    ln_rows(x_s, 0, rows[0])
    ln_rows(x_s, 0, rows[1])
    every = pl.ds(0, T)
    heads(0, 0, every, T)
    heads(0, 2, every, T)
    scores(rows[0], every)
    heads(0, 1, every, T)
    mix(rows[0])
    do_up(0, rows[0])
    pl.semaphore_wait(barrier, 2)
    for b in range(NB):
        emit_block(0, 0, b, mlp_block(0, 0, rows[0], b) + attn_block(0, 0, rows[0], b))
        if b >= 1:
            cross_block(0, 0, b - 1)
    for (name, l), cp in wcopies.items():
        if l == 1:
            cp.start()
    scores(rows[1], every)
    cross_block(0, 0, NB - 1)
    mix(rows[1])
    do_up(0, rows[1])
    for b in range(NB):
        emit_block(0, 1, b, mlp_block(0, 1, rows[1], b) + attn_block(0, 1, rows[1], b))
        if b >= 1:
            cross_block(0, 1, b - 1)
    cross_block(0, 1, NB - 1)

    for b in range(NB):
        finish_block(0, 0, b)
    for b in range(NB):
        f_rdma(0, 0, b).wait_recv()
    y0 = y_s.at[0]
    ln_rows(y0, 1, rows[0])
    for kind in range(3):
        heads(1, kind, rows[0], CH)
    scores(rows[0], rows[0])
    do_up(1, rows[0])
    for b in range(NB):
        acc_s[0, :, pl.ds(*COLS[b])] = mlp_block(1, 0, rows[0], b)
    for b in range(NB):
        finish_block(0, 1, b)
    for b in range(NB):
        f_rdma(0, 1, b).wait_recv()
    ln_rows(y0, 1, rows[1])
    heads(1, 0, rows[1], CH)
    scores(rows[0], rows[1])
    heads(1, 1, rows[1], CH)
    mix(rows[0])
    for b in range(NB):
        emit_block(1, 0, b, acc_s[0, :, pl.ds(*COLS[b])] + attn_block(1, 0, rows[0], b))
        if b >= 1:
            cross_block(1, 0, b - 1)
    heads(1, 2, rows[1], CH)
    scores(rows[1], every)
    cross_block(1, 0, NB - 1)
    mix(rows[1])
    do_up(1, rows[1])
    for b in range(NB):
        emit_block(1, 1, b, mlp_block(1, 1, rows[1], b) + attn_block(1, 1, rows[1], b))
        if b >= 1:
            cross_block(1, 1, b - 1)
    cross_block(1, 1, NB - 1)

    for c in range(2):
        for b in range(NB):
            finish_block(1, c, b)
        for b in range(NB):
            n0, nn = COLS[b]
            f_rdma(1, c, b).wait_recv()
            r = pl.ds(pl.multiple_of(c * CH + (1 - core) * OWN, OWN), OWN)
            out_ref[0, r, pl.ds(n0, nn)] = y_s[1, r, pl.ds(n0, nn)]
    for l in range(2):
        for c in range(2):
            for b in range(NB):
                d_rdma(l, c, b).wait_send()
                x_rdma(l, c, b).wait_send()
                f_rdma(l, c, b).wait_send()


def solution(mesh):
    col_spec = P(None, None, "tp")
    row_spec = P(None, "tp", None)
    in_specs = (P("dp", None, None), P(), col_spec, col_spec, col_spec, P(), P(), row_spec, P(), col_spec, P(None, "tp"), row_spec, P())
    any_spec = pl.BlockSpec(memory_space=pl.ANY)
    vmem_spec = pl.BlockSpec(memory_space=pltpu.VMEM)
    nw = 2 * (3 + len(UPB) + 2 * NB)
    call = pl.pallas_call(
        kernel,
        out_shape=pltpu.VMEM((1, T, D), BF16),
        in_specs=[any_spec] * 13,
        out_specs=vmem_spec,
        scratch_shapes=[
            pltpu.VMEM((2, D), BF16),
            pltpu.VMEM((2, HD), BF16),
            pltpu.VMEM((2, HD), BF16),
            pltpu.VMEM((2, D), BF16),
            pltpu.VMEM((2, FF), BF16),
            pltpu.VMEM((2, D), BF16),
            pltpu.VMEM((T, D), BF16),
            pltpu.VMEM((2, 3 * HW, D), BF16),
            pltpu.VMEM((2, HW, D), BF16),
            pltpu.VMEM((2, D, FF), BF16),
            pltpu.VMEM((2, FF, D), BF16),
            pltpu.VMEM((T, D), BF16),
            pltpu.VMEM((512, CH), F32),
            pltpu.VMEM((NH, T, CH), F32),
            pltpu.VMEM((NH, T, CH), BF16),
            pltpu.VMEM((NH, 128, T), BF16),
            pltpu.VMEM((NH, T, 128), BF16),
            pltpu.VMEM((NH, HD, T), BF16),
            pltpu.VMEM((T, 512), BF16),
            pltpu.VMEM((T, FF), BF16),
            pltpu.VMEM((2, CH, D), F32),
            pltpu.VMEM((2, 2, OWN, D), BF16),
            pltpu.VMEM((2, 2, OWN, D), BF16),
            pltpu.VMEM((2, 2, OWN, D), BF16),
            pltpu.VMEM((2, 2, OWN, D), BF16),
            pltpu.VMEM((2, T, D), BF16),
            pltpu.SemaphoreType.DMA((nw,)),
            pltpu.SemaphoreType.DMA((7,)),
            pltpu.SemaphoreType.DMA((2, 2, NB)),
            pltpu.SemaphoreType.DMA((2, 2, NB)),
            pltpu.SemaphoreType.DMA((2, 2, NB)),
            pltpu.SemaphoreType.DMA((2, 2, NB)),
            pltpu.SemaphoreType.DMA((2, 2, NB)),
            pltpu.SemaphoreType.DMA((2, 2, NB)),
        ],
        compiler_params=pltpu.CompilerParams(collective_id=0, has_side_effects=True, vmem_limit_bytes=54 * 1024 * 1024),
        name="vit_pair",
    )

    def per_device(x, lns, wq, wk, wv, *rest):
        return call(x, lns, *(jnp.swapaxes(w, 1, 2) for w in (wq, wk, wv)), *rest)

    return jax.shard_map(per_device, mesh=mesh, in_specs=in_specs, out_specs=P("dp", None, None), check_vma=False)
```
